32 devices in a mesh: replica: 4 (over z), fsdp: 8 (over y, x, core).
Axes of the slice: x: 2, y: 2, z: 4, core: 2. Of those that a mesh axis runs over, the one named last changes fastest.
Arguments:
- states: bfloat16 [32, 256, 2048], P(('replica', 'fsdp'))
- cotangent: bfloat16 [32, 256, 512], P(('replica', 'fsdp')), may hold values from -6 to 6
- kv_weight: bfloat16 [2048, 512], P('fsdp'), may hold values from -0.125 to 0.125
- norm_gain: bfloat16 [2048], P('fsdp'), may hold values from -1.5 to 1.5
- prompt_len: int32 [32], P(('replica', 'fsdp')), may hold values from 1 to 255, as said below
- response_len: int32 [32], P(('replica', 'fsdp')), may hold values from 1 to 192
- reward_bucket: int32 [32], P(('replica', 'fsdp')), may hold values from 0 to 10, as said below
Outputs:
- key_values: bfloat16 [32, 256, 512], P(('replica', 'fsdp'))
- grad_weight: float32 [2048, 512], P('fsdp')
- grad_gain: float32 [2048], P('fsdp')
The draws below stay inside these ranges and needn't reach their ends.
Inputs may be any that keep to these rules, and one draw needn't show every extreme that they name: prompt_len + response_len <= 256 for every rollout. `reward_bucket`: some rollout has level 0 and some has level 10.
All inputs are finite; a program needn't handle non-finite values.
Results may differ from the reference program's by a relative error of at most 0.005.
Values may be sent and summed in bfloat16 or wider, within the bound.
A program may use at most 64 MiB of HBM per device.

```python
import math
import jax
import jax.numpy as jnp
from jax import lax

D = 2048
KV = 512
SEQ = 256
BUCKETS = 11
ROLLOUTS = 32


def lengths_pair(key):
    salted = jax.random.fold_in(key, 101)
    key_length, key_prompt = jax.random.split(salted)
    rollout_index = jnp.arange(ROLLOUTS, dtype=jnp.int32)
    ceiling = SEQ // 4 + SEQ // 2 * rollout_index // max(ROLLOUTS - 1, 1)
    response = 1 + jax.random.randint(key_length, (ROLLOUTS,), 0, ceiling, dtype=jnp.int32)
    response = response.at[ROLLOUTS - 1].set(SEQ // 4 + SEQ // 2).at[0].set(1)
    prompt = 1 + jax.random.randint(key_prompt, (ROLLOUTS,), 0, SEQ - response, dtype=jnp.int32)
    prompt = prompt.at[0].set(SEQ - 1)
    return (prompt, response)


def draw_prompt_len(key, part):
    return lengths_pair(key)[0]


def draw_response_len(key, part):
    return lengths_pair(key)[1]


def draw_reward_bucket(key, part):
    salted = jax.random.fold_in(key, 202)
    rollout_index = jnp.arange(ROLLOUTS, dtype=jnp.int32)
    ceiling = BUCKETS // 3 + (BUCKETS - BUCKETS // 3) * rollout_index // max(ROLLOUTS - 1, 1)
    levels = jax.random.randint(salted, (ROLLOUTS,), 0, ceiling, dtype=jnp.int32)
    return levels.at[0].set(0).at[ROLLOUTS - 1].set(BUCKETS - 1)


def draw_states(key, part):
    salted = jax.random.fold_in(key, 303)
    key_base, key_rows, key_columns = jax.random.split(salted, 3)
    base = jax.random.normal(key_base, (ROLLOUTS, SEQ, D), jnp.float32)
    row_scale = jnp.exp(jax.random.uniform(key_rows, (ROLLOUTS, SEQ, 1), jnp.float32, math.log(0.3), math.log(3.0)))
    column_scale = jnp.exp(jax.random.uniform(key_columns, (1, 1, D), jnp.float32, math.log(0.3), math.log(3.0)))
    return (base * row_scale * column_scale).astype(jnp.bfloat16)


def steps_of(own_key, extent, cuts, smallest, largest):
    factor_of = 1.0
    for dim, blocks in cuts:
        steps = jax.random.uniform(jax.random.fold_in(jax.random.fold_in(own_key, 6), dim), (blocks,), jnp.float32, smallest / len(cuts), largest / len(cuts))
        factor_of = factor_of * jnp.repeat(jnp.exp(steps), extent[dim] // blocks).reshape((-1,) + (1,) * (len(extent) - 1 - dim))
    return factor_of


def scatter_about(rng, extent, deviation, most, cuts=(), kind=jnp.bfloat16):
    array = deviation * jax.random.normal(rng, extent, jnp.float32)
    if cuts:
        array = array * steps_of(rng, extent, cuts, -0.22, 0.18)
    return jnp.clip(array, -most, most).astype(kind)


def setup_inputs(seed: int = 0) -> dict:
    arg_keys = jax.random.split(jax.random.key(seed), 8)
    return {
        "states": draw_states(jax.random.fold_in(arg_keys[7], 71), 0),
        "cotangent": scatter_about(arg_keys[1], (ROLLOUTS, SEQ, KV), 1.0, 6.0, ((0, 32),)),
        "kv_weight": scatter_about(arg_keys[2], (D, KV), D ** -0.5, 0.125, ((0, 8),)),
        "norm_gain": scatter_about(arg_keys[3], (D,), 0.3, 1.5, ((0, 8),)),
        "prompt_len": draw_prompt_len(jax.random.fold_in(arg_keys[7], 71), 0),
        "response_len": draw_response_len(jax.random.fold_in(arg_keys[7], 71), 0),
        "reward_bucket": draw_reward_bucket(jax.random.fold_in(arg_keys[7], 71), 0),
    }


EPSILON = 1e-06

def reference(states, cotangent, kv_weight, norm_gain, prompt_len, response_len, reward_bucket):
    rollout_count = states.shape[0]
    seq_rows = states.shape[1]
    width = states.shape[2]
    feature_count = kv_weight.shape[1]
    reward_value = reward_bucket.astype(jnp.float32)
    token_total = jnp.sum(response_len.astype(jnp.float32))
    average = jnp.sum(reward_value) / rollout_count
    variance = jnp.sum(reward_value * reward_value) / rollout_count - average * average
    grad_scale = lax.rsqrt(variance + EPSILON) * lax.rsqrt(token_total)
    gain_wide = norm_gain.astype(jnp.float32)
    position = jnp.arange(seq_rows, dtype=jnp.int32)
    group_size = math.gcd(rollout_count, 64)
    group_count = rollout_count // group_size

    def one_group(totals, pieces):
        grad_weight, grad_gain = totals
        part_states, part_cotangent, part_prompt, part_response, part_reward = pieces
        widened = part_states.astype(jnp.float32)
        unit_rows = widened * lax.rsqrt(lax.optimization_barrier(jnp.mean(widened * widened, axis=-1, keepdims=True)) + EPSILON)
        normed = (unit_rows * (1.0 + gain_wide)).astype(jnp.bfloat16)
        flat_normed = normed.reshape(-1, width)
        key_values = jnp.dot(flat_normed, kv_weight, preferred_element_type=jnp.float32).astype(jnp.bfloat16)
        live_flag = (position[None, :] >= part_prompt[:, None]) & (position[None, :] < part_prompt[:, None] + part_response[:, None])
        coefficient = live_flag.astype(jnp.float32) * (part_reward - average)[:, None] * grad_scale
        weighted = (coefficient[:, :, None] * part_cotangent.astype(jnp.float32)).astype(jnp.bfloat16)
        flat_weighted = weighted.reshape(-1, feature_count)
        grad_weight = grad_weight + jnp.dot(flat_normed.T, flat_weighted, preferred_element_type=jnp.float32)
        backward = jnp.dot(flat_weighted, kv_weight.T, preferred_element_type=jnp.float32)
        grad_gain = grad_gain + lax.optimization_barrier(jnp.sum(unit_rows.reshape(-1, width) * backward, axis=0))
        return ((grad_weight, grad_gain), key_values.reshape(group_size, seq_rows, feature_count))
    start_totals = (jnp.zeros((width, feature_count), jnp.float32), jnp.zeros((width,), jnp.float32))
    grouped = (states.reshape(group_count, group_size, seq_rows, width), cotangent.reshape(group_count, group_size, seq_rows, feature_count), prompt_len.reshape(group_count, group_size), response_len.reshape(group_count, group_size), reward_value.reshape(group_count, group_size))
    (grad_weight, grad_gain), key_values = lax.scan(one_group, start_totals, grouped)
    return (key_values.reshape(rollout_count, seq_rows, feature_count), grad_weight, grad_gain)
```

```python
import functools

import jax
import jax.numpy as jnp
from jax import lax
from jax.experimental import pallas as pl
from jax.experimental.pallas import tpu as pltpu
from jax.sharding import PartitionSpec as P

EPSILON = 1e-06
MESH = pl.DeviceIdType.MESH
BF = jnp.bfloat16
F32 = jnp.float32
TILE = 256


def flip(me, mask):
    out = me
    bit = 0
    while mask >> bit:
        if (mask >> bit) & 1:
            own = lax.rem(lax.div(me, 1 << bit), 2)
            out = out + (1 - 2 * own) * (1 << bit)
        bit += 1
    return out


def offset_of(position, order):
    count = len(order)
    return sum(((position >> (count - 1 - i)) & 1) << order[i] for i in range(count))


def kernel(
    R, F, chunk_rows,
    states_hbm, cot_hbm, weight_hbm, gain_ref, prompt_ref, response_ref, reward_ref,
    kv_ref, gw_ref, gg_ref,
    states, cot, normed, live_cot, inverse, w_rel, w_nat, grad, sending, receiving,
    gain_rel, gain_nat, scal_out, scal_in, zscal, gvec, gg_out, gg_in, gg_row, zgg,
    own, chain_out, chain_in,
    load_sem, send_sem, recv_sem,
):
    r, f = lax.axis_index("replica"), lax.axis_index("fsdp")
    bits = F.bit_length() - 1
    rest = list(range(1, bits))
    orders = ([0] + rest if bits else [], [0] + rest[::-1] if bits else [])
    rows, half = w_rel.shape[2], w_rel.shape[3]
    seq, width = states.shape
    row_parts = rows // chunk_rows
    chunks = 2 * row_parts
    tiles = width // TILE
    counter = [2 * chunks]
    pending = []

    def remote(src, dst, device):
        index = counter[0]
        counter[0] += 1
        copy = pltpu.make_async_remote_copy(
            src_ref=src, dst_ref=dst, send_sem=send_sem.at[index], recv_sem=recv_sem.at[index],
            device_id=device, device_id_type=MESH,
        )
        copy.start()
        pending.append(copy)
        return copy

    def across(bit):
        return (r, flip(f, 1 << bit))

    w_loads = []
    for p in range(2):
        w_loads.append(
            pltpu.make_async_copy(
                weight_hbm.at[:, pl.ds(p * half, half)], w_rel.at[p, 0], load_sem.at[p]
            )
        )
    state_load = pltpu.make_async_copy(states_hbm.at[0], states, load_sem.at[2])
    cot_load = pltpu.make_async_copy(cot_hbm.at[0], cot, load_sem.at[3])
    for copy in w_loads + [state_load, cot_load]:
        copy.start()

    gain_rel[0] = gain_ref[...].astype(F32)
    lane = lax.broadcasted_iota(jnp.int32, (8, 128), 1)
    reward = reward_ref[0].astype(F32)
    tokens = response_ref[0].astype(F32)
    zero = jnp.zeros((8, 128), F32)
    scal = jnp.where(lane == 0, zero + reward, zero)
    scal = jnp.where(lane == 1, zero + reward * reward, scal)
    scal = jnp.where(lane == 2, zero + tokens, scal)

    @pl.when(r == 0)
    def _():
        chain_in[0] = jnp.zeros(chain_in.shape[1:], chain_in.dtype)

    @pl.when(r == R - 1)
    def _():
        chain_in[1] = jnp.zeros(chain_in.shape[1:], chain_in.dtype)

    barrier = pltpu.get_barrier_semaphore()
    for bit in range(bits):
        pl.semaphore_signal(barrier, inc=1, device_id=across(bit), device_id_type=MESH)
    for k in range(1, R):
        pl.semaphore_signal(barrier, inc=1, device_id=(lax.rem(r + k, R), f), device_id_type=MESH)
    pl.semaphore_wait(barrier, bits + R - 1)

    def small_send(step, scal):
        bit = orders[0][bits - 1 - step]
        held = 1 << step
        scal_out[step] = scal
        return (
            remote(gain_rel.at[pl.ds(0, held)], gain_rel.at[pl.ds(held, held)], across(bit)),
            remote(scal_out.at[step], scal_in.at[step], across(bit)),
        )

    def small_wait(step, scal, copies):
        for copy in copies:
            copy.wait_recv()
        return scal + scal_in[step]

    def weight_send(step):
        held = 1 << step
        return [
            remote(
                w_rel.at[p, pl.ds(0, held)], w_rel.at[p, pl.ds(held, held)],
                across(orders[p][bits - 1 - step]),
            )
            for p in range(2)
        ]

    small = small_send(0, scal) if bits else None
    for copy in w_loads:
        copy.wait()
    moving = weight_send(0) if bits else []
    state_load.wait()

    def square_tile(i, total):
        part = states[:, pl.ds(pl.multiple_of(i * TILE, TILE), TILE)].astype(F32)
        return total + jnp.sum(part * part, axis=1, keepdims=True)

    squares = lax.fori_loop(0, tiles, square_tile, jnp.zeros((seq, 1), F32))
    inverse[...] = lax.rsqrt(squares / width + EPSILON)
    cot_load.wait()
    position = lax.broadcasted_iota(jnp.int32, (seq, cot.shape[1]), 0)
    first = prompt_ref[0]
    alive = (position >= first) & (position < first + response_ref[0])
    live_cot[...] = jnp.where(alive, cot[...].astype(F32), 0.0).astype(BF)

    for step in range(bits):
        scal = small_wait(step, scal, small)
        if step + 1 < bits:
            small = small_send(step + 1, scal)
        if step == 0 and bits > 1:
            for copy in moving:
                copy.wait_recv()
            moving = weight_send(1)

    scal_out[bits] = scal
    zcopies = [
        remote(scal_out.at[bits], zscal.at[k - 1], (lax.rem(r + k, R), f)) for k in range(1, R)
    ]
    for q in range(F):
        gain_nat[flip(f, offset_of(q, orders[0]))] = gain_rel[q]
    for b in range(F):
        gvec[:, b * rows:(b + 1) * rows] = gain_nat[b]

    def grad_tile(i, carry):
        at = pl.ds(pl.multiple_of(i * TILE, TILE), TILE)
        unit = states[:, at].astype(F32) * inverse[...]
        part = (unit * (1.0 + gvec[:, at])).astype(BF)
        normed[:, at] = part
        grad[at, :] = lax.dot_general(
            part, live_cot[...], (((0,), (0,)), ((), ())), preferred_element_type=F32
        )
        return carry

    lax.fori_loop(0, tiles, grad_tile, 0)

    for copy in zcopies:
        copy.wait_recv()
    for k in range(R - 1):
        scal = scal + zscal[k]
    count = float(R * F)

    def pick(which):
        return jnp.sum(jnp.where(lane[0:1] == which, scal[0:1], 0.0), axis=1, keepdims=True)

    average = pick(0) / count
    variance = pick(1) / count - average * average
    coef = (reward - average) * (lax.rsqrt(variance + EPSILON) * lax.rsqrt(pick(2)))

    starts = [F - (F >> i) for i in range(bits + 1)]

    def partial(p, q, step):
        begin = pl.multiple_of(flip(f, offset_of(q, orders[p])) * rows, rows)
        value = grad[pl.ds(begin, rows), p * half:(p + 1) * half] * coef
        for i in range(step):
            value = value + receiving[p, starts[i] + q].astype(F32)
        return value

    def scatter_send(p, step):
        keep = F >> (step + 1)
        for q in range(keep):
            sending[p, starts[step] + q] = partial(p, keep + q, step).astype(BF)
        at = pl.ds(starts[step], keep)
        return remote(sending.at[p, at], receiving.at[p, at], across(orders[p][step]))

    shares = [scatter_send(p, 0) for p in range(2)] if bits else []
    if bits > 1:
        for p in range(2):
            shares[p].wait_recv()
            shares[p] = scatter_send(p, 1)
    for step in range(2, bits):
        for copy in moving:
            copy.wait_recv()
        moving = weight_send(step)
    for p in range(2):
        if bits:
            moving[p].wait_recv()
        for q in range(F):
            begin = pl.multiple_of(flip(f, offset_of(q, orders[p])) * rows, rows)
            w_nat[pl.ds(begin, rows), p * half:(p + 1) * half] = w_rel[p, q]

    def gain_tile(i, carry):
        at = pl.ds(pl.multiple_of(i * TILE, TILE), TILE)
        backward = lax.dot_general(
            live_cot[...], w_nat[at, :], (((1,), (1,)), ((), ())), preferred_element_type=F32
        )
        unit = states[:, at].astype(F32) * inverse[...]
        gvec[:, at] = jnp.sum(unit * backward, axis=0, keepdims=True) * coef
        return carry

    lax.fori_loop(0, tiles, gain_tile, 0)
    for b in range(F):
        gg_out[0, b] = gvec[:, b * rows:(b + 1) * rows]
    gains = remote(gg_out.at[0], gg_in.at[0], across(0)) if bits else None
    kv_ref[0] = jnp.dot(normed[...], w_nat[...], preferred_element_type=F32).astype(BF)

    def gains_next(step):
        gains.wait_recv()
        gg_out[step] = gg_out[step - 1] + gg_in[step - 1]
        if step < bits:
            return remote(gg_out.at[step], gg_in.at[step], across(step))
        return None

    for step in range(2, bits):
        for p in range(2):
            shares[p].wait_recv()
            shares[p] = scatter_send(p, step)
        gains = gains_next(step - 1)

    near = lax.div(2 * r, R)

    def relay(way, c):
        step = 1 - 2 * way
        before, after = r - step, r + step
        has_before = (before >= 0) & (before < R)
        has_after = (after >= 0) & (after < R)
        index = way * chunks + c
        copy = pltpu.make_async_remote_copy(
            src_ref=chain_out.at[way, c], dst_ref=chain_in.at[way, c],
            send_sem=send_sem.at[index], recv_sem=recv_sem.at[index],
            device_id=(lax.rem(after + R, R), f), device_id_type=MESH,
        )

        @pl.when(has_before)
        def _():
            copy.wait_recv()

        @pl.when(has_after)
        def _():
            chain_out[way, c] = (own[c] + chain_in[way, c].astype(F32)).astype(chain_out.dtype)
            copy.start()

        return has_after, copy

    sent = []
    for p in range(2):
        if bits:
            shares[p].wait_recv()
        value = partial(p, 0, bits)
        for k in range(row_parts):
            own[p * row_parts + k] = value[k * chunk_rows:(k + 1) * chunk_rows]
    lead = min(2, chunks)
    for c in range(lead):
        sent.append(relay(near, c))
    if bits > 1:
        gains = gains_next(bits - 1)
    for c in range(chunks):
        sent.append(relay(1 - near, c))
        if c == 0:
            if bits:
                gains_next(bits)
            gg_row[...] = gg_out[bits, f]
            zgains = [
                remote(gg_row, zgg.at[k - 1], (lax.rem(r + k, R), f)) for k in range(1, R)
            ]
        if c + lead < chunks:
            sent.append(relay(near, c + lead))
        p, k = c // row_parts, c % row_parts
        gw_ref[k * chunk_rows:(k + 1) * chunk_rows, p * half:(p + 1) * half] = (
            own[c] + chain_in[0, c].astype(F32) + chain_in[1, c].astype(F32)
        )
    total = gg_row[...]
    for k in range(R - 1):
        zgains[k].wait_recv()
        total = total + zgg[k]
    gg_ref[...] = total
    for copy in pending:
        copy.wait_send()
    for has_after, copy in sent:
        @pl.when(has_after)
        def _(copy=copy):
            copy.wait_send()


def shards(R, F, states, cotangent, kv_weight, norm_gain, prompt_len, response_len, reward_bucket):
    _, seq, width = states.shape
    rows, features = kv_weight.shape
    half = features // 2
    bits = F.bit_length() - 1
    chunk_rows = max(rows // 2, min(rows, 32))
    chunks = 2 * (rows // chunk_rows)
    wire = BF if R <= 4 else F32
    semaphores = 2 * chunks + 7 * bits + 2 * (R - 1)
    zs = max(R - 1, 1)
    bs = max(bits, 1)
    vmem = pl.BlockSpec(memory_space=pltpu.VMEM)
    smem = pl.BlockSpec(memory_space=pltpu.SMEM)
    hbm = pl.BlockSpec(memory_space=pl.ANY)
    key_values, grad_weight, grad_gain = pl.pallas_call(
        functools.partial(kernel, R, F, chunk_rows),
        out_shape=(
            jax.ShapeDtypeStruct((1, seq, features), BF),
            jax.ShapeDtypeStruct((rows, features), F32),
            jax.ShapeDtypeStruct((1, rows), F32),
        ),
        in_specs=[hbm, hbm, hbm, vmem, smem, smem, smem],
        out_specs=(vmem, vmem, vmem),
        scratch_shapes=[
            pltpu.VMEM((seq, width), BF),
            pltpu.VMEM((seq, features), BF),
            pltpu.VMEM((seq, width), BF),
            pltpu.VMEM((seq, features), BF),
            pltpu.VMEM((seq, 1), F32),
            pltpu.VMEM((2, F, rows, half), BF),
            pltpu.VMEM((width, features), BF),
            pltpu.VMEM((width, features), F32),
            pltpu.VMEM((2, F, rows, half), BF),
            pltpu.VMEM((2, F, rows, half), BF),
            pltpu.VMEM((F, 1, rows), F32),
            pltpu.VMEM((F, 1, rows), F32),
            pltpu.VMEM((bits + 1, 8, 128), F32),
            pltpu.VMEM((bs, 8, 128), F32),
            pltpu.VMEM((zs, 8, 128), F32),
            pltpu.VMEM((1, width), F32),
            pltpu.VMEM((bits + 1, F, 1, rows), F32),
            pltpu.VMEM((bs, F, 1, rows), F32),
            pltpu.VMEM((1, rows), F32),
            pltpu.VMEM((zs, 1, rows), F32),
            pltpu.VMEM((chunks, chunk_rows, half), F32),
            pltpu.VMEM((2, chunks, chunk_rows, half), wire),
            pltpu.VMEM((2, chunks, chunk_rows, half), wire),
            pltpu.SemaphoreType.DMA((4,)),
            pltpu.SemaphoreType.DMA((semaphores,)),
            pltpu.SemaphoreType.DMA((semaphores,)),
        ],
        compiler_params=pltpu.CompilerParams(
            collective_id=0, has_side_effects=True, vmem_limit_bytes=56 * 1024 * 1024
        ),
    )(states, cotangent, kv_weight, norm_gain.reshape(1, rows), prompt_len, response_len, reward_bucket)
    return key_values, grad_weight, grad_gain.reshape(rows)


def solution(mesh):
    placed = (
        P(("replica", "fsdp"), None, None),
        P(("replica", "fsdp"), None, None),
        P("fsdp", None),
        P("fsdp"),
        P(("replica", "fsdp")),
        P(("replica", "fsdp")),
        P(("replica", "fsdp")),
    )
    return jax.shard_map(
        functools.partial(shards, mesh.shape["replica"], mesh.shape["fsdp"]),
        mesh=mesh,
        in_specs=placed,
        out_specs=(P(("replica", "fsdp"), None, None), P("fsdp", None), P("fsdp")),
        check_vma=False,
    )
```

```python
import functools

import jax
import jax.numpy as jnp
from jax import lax
from jax.experimental import pallas as pl
from jax.experimental.pallas import tpu as pltpu
from jax.sharding import PartitionSpec as P

EPSILON = 1e-06
MESH = pl.DeviceIdType.MESH
BF = jnp.bfloat16
F32 = jnp.float32
TILE = 256


def flip(me, mask):
    out = me
    bit = 0
    while mask >> bit:
        if (mask >> bit) & 1:
            own = lax.rem(lax.div(me, 1 << bit), 2)
            out = out + (1 - 2 * own) * (1 << bit)
        bit += 1
    return out


def offset_of(position, order):
    count = len(order)
    return sum(((position >> (count - 1 - i)) & 1) << order[i] for i in range(count))


def kernel(
    R, F, chunk_rows,
    states_hbm, cot_hbm, weight_hbm, gain_ref, prompt_ref, response_ref, reward_ref,
    kv_ref, gw_ref, gg_ref,
    states, cot, normed, live_cot, inverse, w_rel, w_nat, grad, sending, receiving,
    gain_rel, gain_nat, scal_out, scal_in, zscal, gvec, gg_out, gg_in, gg_row, zgg,
    own, chain_out, chain_in,
    load_sem, send_sem, recv_sem,
):
    r, f = lax.axis_index("replica"), lax.axis_index("fsdp")
    bits = F.bit_length() - 1
    rest = list(range(1, bits))
    orders = ([0] + rest if bits else [], [0] + rest[::-1] if bits else [])
    rows, half = w_rel.shape[2], w_rel.shape[3]
    seq, width = states.shape
    row_parts = rows // chunk_rows
    chunks = 2 * row_parts
    tiles = width // TILE
    counter = [2 * chunks]
    pending = []

    def remote(src, dst, device):
        index = counter[0]
        counter[0] += 1
        copy = pltpu.make_async_remote_copy(
            src_ref=src, dst_ref=dst, send_sem=send_sem.at[index], recv_sem=recv_sem.at[index],
            device_id=device, device_id_type=MESH,
        )
        copy.start()
        pending.append(copy)
        return copy

    def across(bit):
        return (r, flip(f, 1 << bit))

    w_loads = []
    for p in range(2):
        w_loads.append(
            pltpu.make_async_copy(
                weight_hbm.at[:, pl.ds(p * half, half)], w_rel.at[p, 0], load_sem.at[p]
            )
        )
    state_load = pltpu.make_async_copy(states_hbm.at[0], states, load_sem.at[2])
    cot_load = pltpu.make_async_copy(cot_hbm.at[0], cot, load_sem.at[3])
    for copy in w_loads + [state_load, cot_load]:
        copy.start()

    gain_rel[0] = gain_ref[...].astype(F32)
    lane = lax.broadcasted_iota(jnp.int32, (8, 128), 1)
    reward = reward_ref[0].astype(F32)
    tokens = response_ref[0].astype(F32)
    zero = jnp.zeros((8, 128), F32)
    scal = jnp.where(lane == 0, zero + reward, zero)
    scal = jnp.where(lane == 1, zero + reward * reward, scal)
    scal = jnp.where(lane == 2, zero + tokens, scal)

    @pl.when(r == 0)
    def _():
        chain_in[0] = jnp.zeros(chain_in.shape[1:], chain_in.dtype)

    @pl.when(r == R - 1)
    def _():
        chain_in[1] = jnp.zeros(chain_in.shape[1:], chain_in.dtype)

    barrier = pltpu.get_barrier_semaphore()
    for bit in range(bits):
        pl.semaphore_signal(barrier, inc=1, device_id=across(bit), device_id_type=MESH)
    for k in range(1, R):
        pl.semaphore_signal(barrier, inc=1, device_id=(lax.rem(r + k, R), f), device_id_type=MESH)
    pl.semaphore_wait(barrier, bits + R - 1)

    def small_send(step, scal):
        bit = orders[0][bits - 1 - step]
        held = 1 << step
        scal_out[step] = scal
        return (
            remote(gain_rel.at[pl.ds(0, held)], gain_rel.at[pl.ds(held, held)], across(bit)),
            remote(scal_out.at[step], scal_in.at[step], across(bit)),
        )

    def small_wait(step, scal, copies):
        for copy in copies:
            copy.wait_recv()
        return scal + scal_in[step]

    def weight_send(step):
        held = 1 << step
        return [
            remote(
                w_rel.at[p, pl.ds(0, held)], w_rel.at[p, pl.ds(held, held)],
                across(orders[p][bits - 1 - step]),
            )
            for p in range(2)
        ]

    small = small_send(0, scal) if bits else None
    for copy in w_loads:
        copy.wait()
    moving = weight_send(0) if bits else []
    state_load.wait()

    def square_tile(i, total):
        part = states[:, pl.ds(pl.multiple_of(i * TILE, TILE), TILE)].astype(F32)
        return total + jnp.sum(part * part, axis=1, keepdims=True)

    squares = lax.fori_loop(0, tiles, square_tile, jnp.zeros((seq, 1), F32))
    inverse[...] = lax.rsqrt(squares / width + EPSILON)
    cot_load.wait()
    position = lax.broadcasted_iota(jnp.int32, (seq, cot.shape[1]), 0)
    first = prompt_ref[0]
    alive = (position >= first) & (position < first + response_ref[0])
    live_cot[...] = jnp.where(alive, cot[...].astype(F32), 0.0).astype(BF)

    for step in range(bits):
        scal = small_wait(step, scal, small)
        if step + 1 < bits:
            small = small_send(step + 1, scal)
        if step == 0 and bits > 1:
            for copy in moving:
                copy.wait_recv()
            moving = weight_send(1)

    scal_out[bits] = scal
    zcopies = [
        remote(scal_out.at[bits], zscal.at[k - 1], (lax.rem(r + k, R), f)) for k in range(1, R)
    ]
    for q in range(F):
        gain_nat[flip(f, offset_of(q, orders[0]))] = gain_rel[q]
    for b in range(F):
        gvec[:, b * rows:(b + 1) * rows] = gain_nat[b]

    def grad_tile(i, carry):
        at = pl.ds(pl.multiple_of(i * TILE, TILE), TILE)
        unit = states[:, at].astype(F32) * inverse[...]
        part = (unit * (1.0 + gvec[:, at])).astype(BF)
        normed[:, at] = part
        grad[at, :] = lax.dot_general(
            part, live_cot[...], (((0,), (0,)), ((), ())), preferred_element_type=F32
        )
        return carry

    lax.fori_loop(0, tiles, grad_tile, 0)

    for copy in zcopies:
        copy.wait_recv()
    for k in range(R - 1):
        scal = scal + zscal[k]
    count = float(R * F)

    def pick(which):
        return jnp.sum(jnp.where(lane[0:1] == which, scal[0:1], 0.0), axis=1, keepdims=True)

    average = pick(0) / count
    variance = pick(1) / count - average * average
    coef = (reward - average) * (lax.rsqrt(variance + EPSILON) * lax.rsqrt(pick(2)))

    starts = [F - (F >> i) for i in range(bits + 1)]

    def partial(p, q, step):
        begin = pl.multiple_of(flip(f, offset_of(q, orders[p])) * rows, rows)
        value = grad[pl.ds(begin, rows), p * half:(p + 1) * half] * coef
        for i in range(step):
            value = value + receiving[p, starts[i] + q].astype(F32)
        return value

    def scatter_send(p, step):
        keep = F >> (step + 1)
        for q in range(keep):
            sending[p, starts[step] + q] = partial(p, keep + q, step).astype(BF)
        at = pl.ds(starts[step], keep)
        return remote(sending.at[p, at], receiving.at[p, at], across(orders[p][step]))

    shares = [scatter_send(p, 0) for p in range(2)] if bits else []
    if bits > 1:
        for p in range(2):
            shares[p].wait_recv()
            shares[p] = scatter_send(p, 1)
    for step in range(2, bits):
        for copy in moving:
            copy.wait_recv()
        moving = weight_send(step)
    for p in range(2):
        if bits:
            moving[p].wait_recv()
        for q in range(F):
            begin = pl.multiple_of(flip(f, offset_of(q, orders[p])) * rows, rows)
            w_nat[pl.ds(begin, rows), p * half:(p + 1) * half] = w_rel[p, q]

    def gain_tile(i, carry):
        at = pl.ds(pl.multiple_of(i * TILE, TILE), TILE)
        backward = lax.dot_general(
            live_cot[...], w_nat[at, :], (((1,), (1,)), ((), ())), preferred_element_type=F32
        )
        unit = states[:, at].astype(F32) * inverse[...]
        gvec[:, at] = jnp.sum(unit * backward, axis=0, keepdims=True) * coef
        return carry

    lax.fori_loop(0, tiles, gain_tile, 0)
    for b in range(F):
        gg_out[0, b] = gvec[:, b * rows:(b + 1) * rows]
    gains = remote(gg_out.at[0], gg_in.at[0], across(0)) if bits else None
    kv_ref[0] = jnp.dot(normed[...], w_nat[...], preferred_element_type=F32).astype(BF)

    def gains_next(step):
        gains.wait_recv()
        gg_out[step] = gg_out[step - 1] + gg_in[step - 1]
        if step < bits:
            return remote(gg_out.at[step], gg_in.at[step], across(step))
        return None

    for step in range(2, bits):
        for p in range(2):
            shares[p].wait_recv()
            shares[p] = scatter_send(p, step)
        gains = gains_next(step - 1)

    near = lax.div(2 * r, R)

    def relay(way, c):
        step = 1 - 2 * way
        before, after = r - step, r + step
        has_before = (before >= 0) & (before < R)
        has_after = (after >= 0) & (after < R)
        index = way * chunks + c
        copy = pltpu.make_async_remote_copy(
            src_ref=chain_out.at[way, c], dst_ref=chain_in.at[way, c],
            send_sem=send_sem.at[index], recv_sem=recv_sem.at[index],
            device_id=(lax.rem(after + R, R), f), device_id_type=MESH,
        )

        @pl.when(has_before)
        def _():
            copy.wait_recv()

        @pl.when(has_after)
        def _():
            chain_out[way, c] = (own[c] + chain_in[way, c].astype(F32)).astype(chain_out.dtype)
            copy.start()

        return has_after, copy

    sent = []
    for p in range(2):
        if bits:
            shares[p].wait_recv()
        value = partial(p, 0, bits)
        for k in range(row_parts):
            own[p * row_parts + k] = value[k * chunk_rows:(k + 1) * chunk_rows]
    lead = chunks
    for c in range(lead):
        sent.append(relay(near, c))
    if bits > 1:
        gains = gains_next(bits - 1)
    for c in range(chunks):
        sent.append(relay(1 - near, c))
        if c == 0:
            if bits:
                gains_next(bits)
            gg_row[...] = gg_out[bits, f]
            zgains = [
                remote(gg_row, zgg.at[k - 1], (lax.rem(r + k, R), f)) for k in range(1, R)
            ]
        if c + lead < chunks:
            sent.append(relay(near, c + lead))
        p, k = c // row_parts, c % row_parts
        gw_ref[k * chunk_rows:(k + 1) * chunk_rows, p * half:(p + 1) * half] = (
            own[c] + chain_in[0, c].astype(F32) + chain_in[1, c].astype(F32)
        )
    total = gg_row[...]
    for k in range(R - 1):
        zgains[k].wait_recv()
        total = total + zgg[k]
    gg_ref[...] = total
    for copy in pending:
        copy.wait_send()
    for has_after, copy in sent:
        @pl.when(has_after)
        def _(copy=copy):
            copy.wait_send()


def shards(R, F, states, cotangent, kv_weight, norm_gain, prompt_len, response_len, reward_bucket):
    _, seq, width = states.shape
    rows, features = kv_weight.shape
    half = features // 2
    bits = F.bit_length() - 1
    chunk_rows = max(rows // 2, min(rows, 32))
    chunks = 2 * (rows // chunk_rows)
    wire = BF if R <= 4 else F32
    semaphores = 2 * chunks + 7 * bits + 2 * (R - 1)
    zs = max(R - 1, 1)
    bs = max(bits, 1)
    vmem = pl.BlockSpec(memory_space=pltpu.VMEM)
    smem = pl.BlockSpec(memory_space=pltpu.SMEM)
    hbm = pl.BlockSpec(memory_space=pl.ANY)
    key_values, grad_weight, grad_gain = pl.pallas_call(
        functools.partial(kernel, R, F, chunk_rows),
        out_shape=(
            jax.ShapeDtypeStruct((1, seq, features), BF),
            jax.ShapeDtypeStruct((rows, features), F32),
            jax.ShapeDtypeStruct((1, rows), F32),
        ),
        in_specs=[hbm, hbm, hbm, vmem, smem, smem, smem],
        out_specs=(vmem, vmem, vmem),
        scratch_shapes=[
            pltpu.VMEM((seq, width), BF),
            pltpu.VMEM((seq, features), BF),
            pltpu.VMEM((seq, width), BF),
            pltpu.VMEM((seq, features), BF),
            pltpu.VMEM((seq, 1), F32),
            pltpu.VMEM((2, F, rows, half), BF),
            pltpu.VMEM((width, features), BF),
            pltpu.VMEM((width, features), F32),
            pltpu.VMEM((2, F, rows, half), BF),
            pltpu.VMEM((2, F, rows, half), BF),
            pltpu.VMEM((F, 1, rows), F32),
            pltpu.VMEM((F, 1, rows), F32),
            pltpu.VMEM((bits + 1, 8, 128), F32),
            pltpu.VMEM((bs, 8, 128), F32),
            pltpu.VMEM((zs, 8, 128), F32),
            pltpu.VMEM((1, width), F32),
            pltpu.VMEM((bits + 1, F, 1, rows), F32),
            pltpu.VMEM((bs, F, 1, rows), F32),
            pltpu.VMEM((1, rows), F32),
            pltpu.VMEM((zs, 1, rows), F32),
            pltpu.VMEM((chunks, chunk_rows, half), F32),
            pltpu.VMEM((2, chunks, chunk_rows, half), wire),
            pltpu.VMEM((2, chunks, chunk_rows, half), wire),
            pltpu.SemaphoreType.DMA((4,)),
            pltpu.SemaphoreType.DMA((semaphores,)),
            pltpu.SemaphoreType.DMA((semaphores,)),
        ],
        compiler_params=pltpu.CompilerParams(
            collective_id=0, has_side_effects=True, vmem_limit_bytes=56 * 1024 * 1024
        ),
    )(states, cotangent, kv_weight, norm_gain.reshape(1, rows), prompt_len, response_len, reward_bucket)
    return key_values, grad_weight, grad_gain.reshape(rows)


def solution(mesh):
    placed = (
        P(("replica", "fsdp"), None, None),
        P(("replica", "fsdp"), None, None),
        P("fsdp", None),
        P("fsdp"),
        P(("replica", "fsdp")),
        P(("replica", "fsdp")),
        P(("replica", "fsdp")),
    )
    return jax.shard_map(
        functools.partial(shards, mesh.shape["replica"], mesh.shape["fsdp"]),
        mesh=mesh,
        in_specs=placed,
        out_specs=(P(("replica", "fsdp"), None, None), P("fsdp", None), P("fsdp")),
        check_vma=False,
    )
```
